16 devices in a mesh: dp: 4 (over y, z, core), tp: 4 (over x).
Axes of the slice: x: 4, y: 2, z: 1, core: 2. Of those that a mesh axis runs over, the one named last changes fastest.
The devices are a block of a 4x4x4 slice.
Arguments:
- x: bfloat16 [256, 7168], P('dp'), parts along dimension 0
- k_cache: bfloat16 [256, 2048, 8, 128], P('dp', None, 'tp'), parts along dimension 0
- v_cache: bfloat16 [256, 2048, 8, 128], P('dp', None, 'tp'), parts along dimension 0
- gain_a: bfloat16 [7168], replicated
- wq: bfloat16 [7168, 7168], P(None, 'tp')
- wo: bfloat16 [7168, 7168], P('tp')
- gain_m: bfloat16 [7168], replicated
- w_gate: bfloat16 [7168, 20480], P(None, 'tp')
- w_up: bfloat16 [7168, 20480], P(None, 'tp')
- w_down: bfloat16 [20480, 7168], P('tp')
Outputs:
- output: bfloat16 [256, 7168], P('dp'), parts along dimension 0
There are 4 independent parts. The reference program is written for one: setup_inputs(seed, part) draws one part's arguments, and reference() takes and returns one part's arrays. A program takes and returns all parts, laid end to end along the dimension named above; an argument that names none is the same for every part.
All inputs are finite; a program needn't handle non-finite values.
Results may differ from the reference program's by a relative error of at most 0.017.
Values are sent between devices in bfloat16 or wider.
A program may use at most 1.5 GiB of HBM per device.

```python
import jax
import jax.numpy as jnp
from jax import lax

BATCH = 64
CACHE = 2048
D = 7168
HEADS = 56
KV_HEADS = 8
HEAD = 128
FF = 20480
THETA = 10000


def setup_inputs(seed: int = 0, part: int = 0) -> dict:
    kx, kc, kw, kn, kq, ko, km, kg, ku, kd = jax.random.split(jax.random.key(seed), 10)
    kx, kc, kw = (jax.random.fold_in(k, part) for k in (kx, kc, kw))

    def weights(key, rows, columns):
        return jax.random.normal(key, (rows, columns), jnp.float32) * rows**-0.5

    drawn = {
        "x": jax.random.normal(kx, (BATCH, D), jnp.float32),
        "k_cache": 2 * jax.random.normal(kc, (BATCH, CACHE, KV_HEADS, HEAD), jnp.float32),
        "v_cache": 4 * jax.random.normal(kw, (BATCH, CACHE, KV_HEADS, HEAD), jnp.float32),
        "gain_a": 1 + 0.1 * jax.random.normal(kn, (D,), jnp.float32),
        "wq": 2 * weights(kq, D, HEADS * HEAD),
        "wo": weights(ko, HEADS * HEAD, D),
        "gain_m": 1 + 0.1 * jax.random.normal(km, (D,), jnp.float32),
        "w_gate": weights(kg, D, FF),
        "w_up": weights(ku, D, FF),
        "w_down": 2 * weights(kd, FF, D),
    }
    return {k: v.astype(jnp.bfloat16) for k, v in drawn.items()}


def normed(x, gain):
    wide = x.astype(jnp.float32)
    scale = lax.rsqrt(jnp.mean(wide * wide, -1, keepdims=True) + 1e-6)
    return (wide * scale * gain.astype(jnp.float32)).astype(jnp.bfloat16)


def turned(t, place, theta):
    half = t.shape[-1] // 2
    angle = place.astype(jnp.float32)[:, None] * theta ** (-jnp.arange(half, dtype=jnp.float32) / half)
    cos, sin = jnp.cos(angle)[:, None], jnp.sin(angle)[:, None]
    a, b = t[..., :half].astype(jnp.float32), t[..., half:].astype(jnp.float32)
    return jnp.concatenate([a * cos - b * sin, b * cos + a * sin], -1).astype(jnp.bfloat16)


def matmul(a, w):
    return jnp.dot(a, w, preferred_element_type=jnp.float32).astype(jnp.bfloat16)


def einsum(form, a, b):
    return jnp.einsum(form, a.astype(jnp.float32), b.astype(jnp.float32))


def seen_by(a, wq, k_cache, v_cache, head, theta):
    batch, cache, kv_heads = k_cache.shape[:3]
    place = jnp.full((batch,), cache - 1)
    q = turned(matmul(a, wq).reshape(batch, -1, head), place, theta).reshape(batch, kv_heads, -1, head)
    scores = einsum("bgsd,bugd->bgsu", q, k_cache) * head**-0.5
    weights = jax.nn.softmax(scores, -1).astype(jnp.bfloat16)
    return einsum("bgsu,bugd->bgsd", weights, v_cache).astype(jnp.bfloat16).reshape(batch, -1)


def hidden_of(b, w_gate, w_up):
    gate = jnp.dot(b, w_gate, preferred_element_type=jnp.float32)
    up = jnp.dot(b, w_up, preferred_element_type=jnp.float32)
    return (jax.nn.silu(gate) * up).astype(jnp.bfloat16)


def reference(x, k_cache, v_cache, gain_a, wq, wo, gain_m, w_gate, w_up, w_down):
    seen = seen_by(normed(x, gain_a), wq, k_cache, v_cache, HEAD, THETA)
    h = (x.astype(jnp.float32) + jnp.dot(seen, wo, preferred_element_type=jnp.float32)).astype(jnp.bfloat16)
    hidden = hidden_of(normed(h, gain_m), w_gate, w_up)
    return (h.astype(jnp.float32) + jnp.dot(hidden, w_down, preferred_element_type=jnp.float32)).astype(jnp.bfloat16)
```

```python
import functools

import jax
import jax.numpy as jnp
import numpy as np
from jax import lax
from jax.experimental import pallas as pl
from jax.experimental.pallas import tpu as pltpu
from jax.sharding import PartitionSpec as P

HEAD = 128
THETA = 10000
MESH = pl.DeviceIdType.MESH
BN = 256
PAD = 16
F32, BF16 = jnp.float32, jnp.bfloat16


def rows(at, size, step=16):
    return pl.ds(pl.multiple_of(at, step), size)


def product(a, w, depth, piece):
    total = None
    for k in range(0, depth, piece):
        term = jnp.dot(a(k, piece), w(k, piece), preferred_element_type=F32)
        total = term if total is None else total + term
    return total


def kernel(cfg, x_hbm, k_hbm, v_hbm, ga_ref, wq_hbm, wo_hbm, gm_ref, wg_hbm, wu_hbm, wd_hbm, turn_ref, y_ref,
           arena, x_ref, norm, qt, qs, os_, seen, terms, got, own, hb, hid, yb, sc,
           blk_sem, kv_sem, x_sem, rs_send, rs_recv, ag_send, ag_recv, rs2_send, rs2_recv, ag2_send, ag2_recv):
    n, batch, d, keys, heads, ff, chunks, reduce_at = (
        cfg["n"], cfg["batch"], cfg["d"], cfg["keys"], cfg["heads"], cfg["ff"], cfg["chunks"], cfg["reduce_at"])
    qw = heads * HEAD
    own_cols = d // n
    groups = own_cols // BN
    half = 7
    wo_at = half * d
    kv_slots = (half * d) // (2 * keys)
    pairs = batch // 2
    n_up = ff // BN
    me = lax.axis_index("tp")
    scale = HEAD ** -0.5

    def peer(rel):
        return {"tp": lax.rem(me + rel, n)}

    barrier = pltpu.get_barrier_semaphore()
    for rel in range(1, n):
        pl.semaphore_signal(barrier, inc=1, device_id=peer(rel), device_id_type=MESH)

    def wq_copy(i):
        return pltpu.make_async_copy(wq_hbm.at[:, rows(i * BN, BN, BN)], arena.at[rows(i * d, d), :], blk_sem.at[i])

    def wo_copy(i):
        return pltpu.make_async_copy(wo_hbm.at[:, rows(i * BN, BN, BN)], arena.at[rows(wo_at + i * qw, qw), :], blk_sem.at[half + i])

    def kv_copies(p):
        slot = lax.rem(p, kv_slots)
        base = slot * (2 * keys)
        return [
            pltpu.make_async_copy(src.at[2 * p + s], arena.at[rows(base + j * keys, keys), s * HEAD:(s + 1) * HEAD], kv_sem.at[slot, 2 * j + s])
            for j, src in enumerate((k_hbm, v_hbm)) for s in range(2)
        ]

    def region(t):
        r = lax.rem(t, 2 * half)
        return (lax.rem(r + 3, half) + half * (r // half)) * d

    def up_copy(j, which):
        src = (wg_hbm, wu_hbm)[which]
        t = 2 * j + which
        return pltpu.make_async_copy(src.at[:, rows(j * BN, BN, BN)], arena.at[rows(region(t), d), :], blk_sem.at[lax.rem(t, 2 * half)])

    def down_copy(e):
        g, q = e // n, lax.rem(e, n)
        col = lax.rem(me + q, n) * groups + g - (n - 1 - q) // (n - 1)
        t = 2 * n_up - 1 + e
        return pltpu.make_async_copy(wd_hbm.at[:, rows(col * BN, BN, BN)], arena.at[rows(region(t), ff), :], blk_sem.at[lax.rem(t, 2 * half)])

    def down_at(e):
        return region(2 * n_up - 1 + e)

    n_wq, n_wo = qw // BN, d // BN
    for i in range(n_wq):
        wq_copy(i).start()
    x_copy = pltpu.make_async_copy(x_hbm, x_ref, x_sem.at[0])
    x_copy.start()

    def columns(c):
        return rows(c * BN, BN, BN)

    def norm_scale(read):
        def add(c, total):
            wide = read(c).astype(F32)
            sq = wide * wide
            return total + sq[:, :128] + sq[:, 128:]
        total = lax.fori_loop(0, d // BN, add, jnp.zeros((batch, 128), F32))
        return lax.rsqrt(jnp.sum(total, -1, keepdims=True) / d + 1e-6)

    def norm_into(read, gain_ref):
        s = norm_scale(read)

        def put(c, _):
            norm[:, columns(c)] = (read(c).astype(F32) * s * gain_ref[:, columns(c)].astype(F32)).astype(BF16)
            return 0
        lax.fori_loop(0, d // BN, put, 0)

    x_copy.wait()
    norm_into(lambda c: x_ref[:, columns(c)], ga_ref)
    qs[...] = jnp.zeros_like(qs)

    def with_norm(at):
        return product(lambda k, m: norm[:, k:k + m], lambda k, m: arena[rows(at + k, m), :], d, d // 4)

    def query(i, _):
        wq_copy(i).wait()
        q = with_norm(i * d).astype(BF16).astype(F32)
        for s in range(BN // HEAD):
            t = q[:, s * HEAD:(s + 1) * HEAD]
            t = t * turn_ref[0:1, :] + pltpu.roll(t, HEAD // 2, 1) * turn_ref[1:2, :]
            qt[i * (BN // HEAD) + s] = t.astype(BF16).astype(F32)

        @pl.when(i >= 1)
        def _():
            for c in kv_copies(i - 1):
                c.start()

        def more(w, _):
            wo_copy(w).start()
            return 0
        lax.fori_loop(i * (n_wo // n_wq), (i + 1) * (n_wo // n_wq), more, 0)
        return 0

    lax.fori_loop(0, n_wq, query, 0)
    for h in range(heads):
        qs[pl.ds(h, batch, stride=PAD), :] = qt[h]

    row = lax.broadcasted_iota(jnp.int32, (2 * PAD, 512), 0)
    lane = lax.broadcasted_iota(jnp.int32, (2 * PAD, 512), 1)
    in_second = (lax.rem(row, PAD) >= heads // 2).astype(jnp.int32)
    bias = jnp.where(lax.rem(lane, 2) == in_second, 0.0, -jnp.inf).astype(F32)
    first = lax.broadcasted_iota(jnp.int32, (2 * PAD, HEAD), 0) < PAD
    pieces = keys // 512

    def attend(p, _):
        copies = kv_copies(p)
        for c in copies:
            c.wait()
        base = lax.rem(p, kv_slots) * (2 * keys)
        q = qs[rows(p * (2 * PAD), 2 * PAD), :]
        q = jnp.concatenate([jnp.where(first, q, 0.0), jnp.where(first, 0.0, q)], 1).astype(BF16)
        top = None
        for c in range(pieces):
            s = lax.dot_general(q, arena[rows(base + c * 512, 512), :], (((1,), (1,)), ((), ())), preferred_element_type=F32)
            s = s * scale + bias
            sc[:, c * 512:(c + 1) * 512] = s
            top = s if top is None else jnp.maximum(top, s)
        top = jnp.max(top, -1, keepdims=True)
        total = None
        for c in range(pieces):
            e = jnp.exp(sc[:, c * 512:(c + 1) * 512] - top)
            sc[:, c * 512:(c + 1) * 512] = e
            total = e if total is None else total + e
        inv = 1.0 / jnp.sum(total, -1, keepdims=True)
        o = None
        for c in range(pieces):
            w = (sc[:, c * 512:(c + 1) * 512] * inv).astype(BF16)
            t = jnp.dot(w, arena[rows(base + keys + c * 512, 512), :], preferred_element_type=F32)
            o = t if o is None else o + t
        os_[rows(p * (2 * PAD), 2 * PAD), :] = jnp.concatenate([o[:PAD, :HEAD], o[PAD:, HEAD:]], 0)

        @pl.when(p + kv_slots < pairs)
        def _():
            for c in kv_copies(p + kv_slots):
                c.start()

        for t, after in enumerate(cfg["after"]):
            @pl.when(p == after)
            def _():
                up_copy(t // 2, t % 2).start()
        return 0

    def rs_copy(c, rel):
        r0, r = chunks[c]
        return pltpu.make_async_remote_copy(
            src_ref=terms.at[rel - 1, :, r0:r0 + r, :], dst_ref=got.at[rel - 1, :, r0:r0 + r, :],
            send_sem=rs_send.at[c, rel - 1], recv_sem=rs_recv.at[c, rel - 1], device_id=peer(rel), device_id_type=MESH)

    def ag_copy(c, rel, owner):
        r0, r = chunks[c]
        return pltpu.make_async_remote_copy(
            src_ref=hb.at[owner, :, r0:r0 + r, :], dst_ref=hb.at[owner, :, r0:r0 + r, :],
            send_sem=ag_send.at[c, rel - 1], recv_sem=ag_recv.at[c, rel - 1], device_id=peer(rel), device_id_type=MESH)

    def project(c):
        r0, r = chunks[c]
        for h in range(heads):
            seen[r0:r0 + r, h * HEAD:(h + 1) * HEAD] = os_[pl.ds(r0 * PAD + h, r, stride=PAD), :].astype(BF16)
        for rel in [*range(1, n), 0]:
            def block(g, _):
                col = lax.rem(me + rel, n) * groups + g
                if c == 0:
                    wo_copy(col).wait()
                t = product(lambda k, m: seen[r0:r0 + r, k:k + m], lambda k, m: arena[rows(wo_at + col * qw + k, m), :], qw, qw)
                if rel:
                    terms[rel - 1, g, r0:r0 + r, :] = t.astype(BF16)
                else:
                    own[g, r0:r0 + r, :] = t
                return 0
            lax.fori_loop(0, groups, block, 0)
            if rel:
                rs_copy(c, rel).start()

    def reduce(c):
        r0, r = chunks[c]
        for rel in range(1, n):
            rs_copy(c, rel).wait_recv()

        def block(g, _):
            s = own[g, r0:r0 + r, :]
            for rel in range(1, n):
                s += got[rel - 1, g, r0:r0 + r, :].astype(F32)
            hb[me, g, r0:r0 + r, :] = (x_ref[r0:r0 + r, rows(me * own_cols + g * BN, BN, BN)].astype(F32) + s).astype(BF16)
            return 0
        lax.fori_loop(0, groups, block, 0)
        for rel in range(1, n):
            ag_copy(c, rel, me).start()

    for c, (r0, r) in enumerate(chunks):
        if c:
            mid = (r0 + reduce_at[c]) // 2
            lax.fori_loop(r0 // 2, mid, attend, 0)
            reduce(c - 1)
            lax.fori_loop(mid, (r0 + r) // 2, attend, 0)
        else:
            lax.fori_loop(r0 // 2, (r0 + r) // 2, attend, 0)
            pl.semaphore_wait(barrier, n - 1)
        project(c)
    for t in range(half, 2 * half):
        up_copy(t // 2, t % 2).start()
    last = len(chunks) - 1
    reduce(last)
    for c in range(len(chunks)):
        for rel in range(1, n):
            rs_copy(c, rel).wait_send()
            ag_copy(c, rel, me).wait_send()
            ag_copy(c, rel, lax.rem(me + n - rel, n)).wait_recv()

    norm_into(lambda c: hb[c // groups, lax.rem(c, groups)], gm_ref)

    def up(j, _):
        up_copy(j, 0).wait()
        gate = with_norm(region(2 * j))
        up_copy(j, 1).wait()
        value = with_norm(region(2 * j + 1))
        hid[:, columns(j)] = (jax.nn.silu(gate) * value).astype(BF16)

        @pl.when(j + half < n_up)
        def _():
            up_copy(j + half, 0).start()
            up_copy(j + half, 1).start()

        @pl.when(j + half >= n_up)
        def _():
            e = 2 * (j + half - n_up) + 1
            down_copy(e).start()
            down_copy(e + 1).start()
        return 0
    lax.fori_loop(0, n_up, up, 0)

    n_down = n * groups

    def down(e):
        down_copy(e).wait()
        at = down_at(e)
        t = product(lambda k, m: hid[:, k:k + m], lambda k, m: arena[rows(at + k, m), :], ff, ff // 4)

        @pl.when(e + 2 * half <= n_down)
        def _():
            down_copy(e + 2 * half).start()
        return t

    def rs2_copy(g, rel):
        return pltpu.make_async_remote_copy(
            src_ref=terms.at[rel - 1, g], dst_ref=got.at[rel - 1, g],
            send_sem=rs2_send.at[rel - 1, g], recv_sem=rs2_recv.at[rel - 1, g], device_id=peer(rel), device_id_type=MESH)

    def ag2_copy(g, rel, owner):
        return pltpu.make_async_remote_copy(
            src_ref=yb.at[owner, g], dst_ref=yb.at[owner, g],
            send_sem=ag2_send.at[rel - 1, g], recv_sem=ag2_recv.at[rel - 1, g], device_id=peer(rel), device_id_type=MESH)

    def finish(g):
        for rel in range(1, n):
            rs2_copy(g, rel).wait_recv()
        s = own[g]
        for rel in range(1, n):
            s += got[rel - 1, g].astype(F32)
        yb[me, g] = (hb[me, g].astype(F32) + s).astype(BF16)
        for rel in range(1, n):
            ag2_copy(g, rel, me).start()

    def group(g, _):
        @pl.when(g >= 1)
        def _():
            own[g - 1] = down(n * g)

        def other(rel, _):
            terms[rel - 1, g] = down(n * g + rel).astype(BF16)
            rs2_copy(g, rel).start()
            return 0
        lax.fori_loop(1, n, other, 0)

        @pl.when(g >= 1)
        def _():
            finish(g - 1)
        return 0

    lax.fori_loop(0, groups, group, 0)
    own[groups - 1] = down(n_down)
    finish(groups - 1)

    def leave(g, _):
        for rel in range(1, n):
            rs2_copy(g, rel).wait_send()
            ag2_copy(g, rel, me).wait_send()
            ag2_copy(g, rel, lax.rem(me + n - rel, n)).wait_recv()
        for o in range(n):
            y_ref[:, rows(o * own_cols + g * BN, BN, BN)] = yb[o, g]
        return 0
    lax.fori_loop(0, groups, leave, 0)


def solution(mesh):
    n = mesh.shape["tp"]

    def step(x, k_cache, v_cache, gain_a, wq, wo, gain_m, w_gate, w_up, w_down):
        batch, d = x.shape
        cache, kv_heads = k_cache.shape[1:3]
        keys = cache * kv_heads
        heads = wq.shape[1] // HEAD
        ff = w_gate.shape[1]
        half, groups = 7, d // n // BN
        kv_slots = half * d // (2 * keys)
        pairs = batch // 2
        after = []
        for t in range(half):
            r = (t + 3) % half
            need = [s for s in range(kv_slots) if s * 2 * keys < (r + 1) * d and (s + 1) * 2 * keys > r * d]
            after.append(max(p for p in range(pairs - kv_slots, pairs) if p % kv_slots in need))
        chunks = ((0, batch * 3 // 4), (batch * 3 // 4, batch // 4))
        cfg = dict(n=n, batch=batch, d=d, keys=keys, heads=heads, ff=ff, chunks=chunks, reduce_at=(0, batch // 8), after=after)

        i = np.arange(HEAD // 2)
        angle = (cache - 1) * THETA ** (-i / (HEAD // 2))
        cos, sin = np.cos(angle), np.sin(angle)
        turn = jnp.asarray(np.stack([np.concatenate([cos, cos]), np.concatenate([-sin, sin])]), F32)

        any_, vmem = pl.BlockSpec(memory_space=pl.ANY), pl.BlockSpec(memory_space=pltpu.VMEM)
        dma = pltpu.SemaphoreType.DMA
        nc = len(chunks)
        return pl.pallas_call(
            functools.partial(kernel, cfg),
            out_shape=jax.ShapeDtypeStruct(x.shape, x.dtype),
            in_specs=[any_, any_, any_, vmem, any_, any_, vmem, any_, any_, any_, vmem],
            out_specs=vmem,
            scratch_shapes=[
                pltpu.VMEM((2 * half * d, BN), BF16),
                pltpu.VMEM((batch, d), BF16),
                pltpu.VMEM((batch, d), BF16),
                pltpu.VMEM((heads, batch, HEAD), F32),
                pltpu.VMEM((batch * PAD, HEAD), F32),
                pltpu.VMEM((batch * PAD, HEAD), F32),
                pltpu.VMEM((batch, heads * HEAD), BF16),
                pltpu.VMEM((n - 1, groups, batch, BN), BF16),
                pltpu.VMEM((n - 1, groups, batch, BN), BF16),
                pltpu.VMEM((groups, batch, BN), F32),
                pltpu.VMEM((n, groups, batch, BN), BF16),
                pltpu.VMEM((batch, ff), BF16),
                pltpu.VMEM((n, groups, batch, BN), BF16),
                pltpu.VMEM((2 * PAD, keys), F32),
                dma((half + d // BN,)), dma((kv_slots, 4)), dma((1,)),
                dma((nc, n - 1)), dma((nc, n - 1)), dma((nc, n - 1)), dma((nc, n - 1)),
                dma((n - 1, groups)), dma((n - 1, groups)), dma((n - 1, groups)), dma((n - 1, groups)),
            ],
            compiler_params=pltpu.CompilerParams(collective_id=0, has_side_effects=True, vmem_limit_bytes=67043328),
        )(x, k_cache.reshape(batch, keys, HEAD), v_cache.reshape(batch, keys, HEAD), gain_a.reshape(1, d), wq, wo,
          gain_m.reshape(1, d), w_gate, w_up, w_down, turn)

    states, cache, columns_, rows_of = P("dp", None), P("dp", None, "tp", None), P(None, "tp"), P("tp", None)
    return jax.shard_map(
        step,
        mesh=mesh,
        in_specs=(states, cache, cache, P(None), columns_, rows_of, P(None), columns_, columns_, rows_of),
        out_specs=states,
        check_vma=False,
    )
```

```python
import functools

import jax
import jax.numpy as jnp
import numpy as np
from jax import lax
from jax.experimental import pallas as pl
from jax.experimental.pallas import tpu as pltpu
from jax.sharding import PartitionSpec as P

HEAD = 128
THETA = 10000
MESH = pl.DeviceIdType.MESH
BN = 256
PAD = 16
F32, BF16 = jnp.float32, jnp.bfloat16


def rows(at, size, step=16):
    return pl.ds(pl.multiple_of(at, step), size)


def product(a, w, depth, piece):
    total = None
    for k in range(0, depth, piece):
        term = jnp.dot(a(k, piece), w(k, piece), preferred_element_type=F32)
        total = term if total is None else total + term
    return total


def products(a, ws, depth, piece):
    totals = [None] * len(ws)
    for k in range(0, depth, piece):
        for i, w in enumerate(ws):
            term = jnp.dot(a(k, piece), w(k, piece), preferred_element_type=F32)
            totals[i] = term if totals[i] is None else totals[i] + term
    return totals


def kernel(cfg, x_hbm, k_hbm, v_hbm, ga_ref, wq_hbm, wo_hbm, gm_ref, wg_hbm, wu_hbm, wd_hbm, turn_ref, y_ref,
           arena, x_ref, norm, qt, qs, os_, seen, far_terms, far_got, side, terms, got, own, hb, hid, yb, sc_a, sc_b,
           blk_sem, kv_sem, x_sem, *link_sems):
    n, batch, d, keys, heads, ff, chunks = cfg["n"], cfg["batch"], cfg["d"], cfg["keys"], cfg["heads"], cfg["ff"], cfg["chunks"]
    qw = heads * HEAD
    own_cols = d // n
    groups = own_cols // BN
    half = 7
    wo_at = half * d
    kv_slots = (half * d) // (2 * keys)
    pairs = batch // 2
    n_up = ff // BN
    me = lax.axis_index("tp")
    scale = HEAD ** -0.5

    FAR, RIGHT, LEFT = 2, 1, n - 1
    to = (RIGHT, LEFT)

    def device(rel):
        return lax.rem(me + rel, n)

    barrier = pltpu.get_barrier_semaphore()
    for rel in range(1, n):
        pl.semaphore_signal(barrier, inc=1, device_id={"tp": device(rel)}, device_id_type=MESH)

    def link(kind, index, way, src, dst, rel=None):
        send, recv = link_sems[2 * kind], link_sems[2 * kind + 1]
        return pltpu.make_async_remote_copy(
            src_ref=src, dst_ref=dst, send_sem=send.at[way, index], recv_sem=recv.at[way, index],
            device_id={"tp": device(to[way] if rel is None else rel)}, device_id_type=MESH)

    def wq_copy(i):
        return pltpu.make_async_copy(wq_hbm.at[:, rows(i * BN, BN, BN)], arena.at[rows(i * d, d), :], blk_sem.at[i])

    def wo_copy(i):
        return pltpu.make_async_copy(wo_hbm.at[:, rows(i * BN, BN, BN)], arena.at[rows(wo_at + i * qw, qw), :], blk_sem.at[half + i])

    def kv_copies(p, kinds=(0, 1)):
        slot = lax.rem(p, kv_slots)
        base = slot * (2 * keys)
        return [
            pltpu.make_async_copy(src.at[2 * p + s], arena.at[rows(base + j * keys, keys), s * HEAD:(s + 1) * HEAD], kv_sem.at[slot, 2 * j + s])
            for j, src in enumerate((k_hbm, v_hbm)) if j in kinds for s in range(2)
        ]

    def region(t):
        r = lax.rem(t, 2 * half)
        return (lax.rem(r + 3, half) + half * (r // half)) * d

    def up_copy(j, which):
        src = (wg_hbm, wu_hbm)[which]
        t = 2 * j + which
        return pltpu.make_async_copy(src.at[:, rows(j * BN, BN, BN)], arena.at[rows(region(t), d), :], blk_sem.at[lax.rem(t, 2 * half)])

    OWN = 0
    half_terms = [(FAR, g) for g in range(groups)] + [(OWN, 0)]
    order = [half_terms[i:i + 2] for i in range(0, groups + 1, 2)]
    for g in range(groups):
        order.append([(RIGHT, g), (LEFT, g)])
        if g % 3 == 1:
            at = g // 3 * 2 + 1
            order.append([(OWN, at), (OWN, at + 1)])
    order.append([(OWN, groups - 2), (OWN, groups - 1)])
    blocks = [b for two in order for b in two]

    def down_copy(v):
        rel, group = blocks[v]
        t = 2 * n_up + v
        src = wd_hbm.at[:, rows((device(rel) * groups + group) * BN, BN, BN)]
        return pltpu.make_async_copy(src, arena.at[rows(region(t), ff), :], blk_sem.at[t % (2 * half)])

    n_wq, n_wo = qw // BN, d // BN
    for i in range(n_wq):
        wq_copy(i).start()
    x_copy = pltpu.make_async_copy(x_hbm, x_ref, x_sem.at[0])
    x_copy.start()

    def columns(c):
        return rows(c * BN, BN, BN)

    def norm_into(read, gain_ref, r0, r):
        def add(o, total):
            for g in range(groups):
                wide = read(o, g).astype(F32)
                sq = wide * wide
                total = total + (sq[:, :128] + sq[:, 128:])
            return total
        total = lax.fori_loop(0, n, add, jnp.zeros((r, 128), F32))
        s = lax.rsqrt(jnp.sum(total, -1, keepdims=True) / d + 1e-6)

        def put(o, _):
            for g in range(groups):
                at = columns(o * groups + g)
                norm[r0:r0 + r, at] = (read(o, g).astype(F32) * s * gain_ref[:, at].astype(F32)).astype(BF16)
            return 0
        lax.fori_loop(0, n, put, 0)

    x_copy.wait()
    norm_into(lambda o, g: x_ref[:, columns(o * groups + g)], ga_ref, 0, batch)
    qs[...] = jnp.zeros_like(qs)

    def with_norm(at):
        return product(lambda k, m: norm[:, k:k + m], lambda k, m: arena[rows(at + k, m), :], d, d // 4)

    def query(i, _):
        wq_copy(i).wait()
        q = with_norm(i * d).astype(BF16).astype(F32)
        for s in range(BN // HEAD):
            t = q[:, s * HEAD:(s + 1) * HEAD]
            t = t * turn_ref[0:1, :] + pltpu.roll(t, HEAD // 2, 1) * turn_ref[1:2, :]
            qt[i * (BN // HEAD) + s] = t.astype(BF16).astype(F32)

        @pl.when(i >= 1)
        def _():
            for c in kv_copies(i - 1):
                c.start()

        def more(w, _):
            wo_copy(w).start()
            return 0
        lax.fori_loop(i * (n_wo // n_wq), (i + 1) * (n_wo // n_wq), more, 0)
        return 0

    lax.fori_loop(0, n_wq, query, 0)
    for h in range(heads):
        qs[pl.ds(h, batch, stride=PAD), :] = qt[h]

    row = lax.broadcasted_iota(jnp.int32, (2 * PAD, 512), 0)
    lane = lax.broadcasted_iota(jnp.int32, (2 * PAD, 512), 1)
    in_second = (lax.rem(row, PAD) >= heads // 2).astype(jnp.int32)
    bias = jnp.where(lax.rem(lane, 2) == in_second, 0.0, -jnp.inf).astype(F32)
    first = lax.broadcasted_iota(jnp.int32, (2 * PAD, HEAD), 0) < PAD
    width = 512

    def kv_base(p):
        return lax.rem(p, kv_slots) * (2 * keys)

    def wait_keys(p):
        for c in kv_copies(p, (0,)):
            c.wait()

    def wait_values(p):
        for c in kv_copies(p, (1,)):
            c.wait()

    def score(p, sc):
        q = qs[rows(p * (2 * PAD), 2 * PAD), :]
        q = jnp.concatenate([jnp.where(first, q, 0.0), jnp.where(first, 0.0, q)], 1).astype(BF16)
        for c in range(0, keys, width):
            s = lax.dot_general(q, arena[rows(kv_base(p) + c, width), :], (((1,), (1,)), ((), ())), preferred_element_type=F32)
            sc[:, c:c + width] = s * scale + bias

    def see(p, sc):
        top = None
        for c in range(0, keys, width):
            s = sc[:, c:c + width]
            top = s if top is None else jnp.maximum(top, s)
        top = jnp.max(top, -1, keepdims=True)
        total = None
        for c in range(0, keys, width):
            e = jnp.exp(sc[:, c:c + width] - top)
            sc[:, c:c + width] = e
            total = e if total is None else total + e
        inv = 1.0 / jnp.sum(total, -1, keepdims=True)
        o = None
        for c in range(0, keys, BN):
            w = (sc[:, c:c + BN] * inv).astype(BF16)
            t = jnp.dot(w, arena[rows(kv_base(p) + keys + c, BN), :], preferred_element_type=F32)
            o = t if o is None else o + t
        os_[rows(p * (2 * PAD), 2 * PAD), :] = jnp.concatenate([o[:PAD, :HEAD], o[PAD:, HEAD:]], 0)

    def two_pairs(i, end):
        p = 2 * i
        wait_keys(p + 1)
        wait_values(p)
        wait_values(p + 1)
        if not end:
            wait_keys(p + 2)
        score(p + 1, sc_b)
        see(p, sc_a)
        if not end:
            score(p + 2, sc_a)
        see(p + 1, sc_b)

        if not end:
            @pl.when(p + 1 + kv_slots < pairs)
            def _():
                for c in kv_copies(p + kv_slots) + kv_copies(p + 1 + kv_slots):
                    c.start()

        for t, after in enumerate(cfg["after"]):
            if end:
                if after // 2 == i:
                    up_copy(t // 2, t % 2).start()
            elif after // 2 < pairs // 2 - 1:
                @pl.when(i == after // 2)
                def _():
                    up_copy(t // 2, t % 2).start()

    def attend(first_row, last_row):
        def step(i, _):
            two_pairs(i, False)
            return 0
        lo, hi = first_row // 4, last_row // 4
        lax.fori_loop(lo, min(hi, pairs // 2 - 1), step, 0)
        if hi == pairs // 2:
            two_pairs(hi - 1, True)

    half_lanes = (slice(0, BN // 2), slice(BN // 2, BN))

    def chunk_link(kind, c, way, owner=None):
        r0, r = chunks[c]
        straight = kind == 3 and c == len(chunks) - 1
        lanes = half_lanes[way] if kind == 3 and not straight else slice(0, BN)
        owner = me if owner is None else owner

        def at(ref, first=way):
            return ref.at[first, :, r0:r0 + r]
        if kind < 2:
            src, dst = ((far_terms, far_got), (terms, got))[kind]
            return link(kind, c, way, at(src), at(dst))
        states = hb.at[owner, :, r0:r0 + r, lanes]
        return link(kind, c, way, states, states, FAR if straight else None)

    def project(c):
        r0, r = chunks[c]
        for h in range(heads):
            seen[r0:r0 + r, h * HEAD:(h + 1) * HEAD] = os_[pl.ds(r0 * PAD + h, r, stride=PAD), :].astype(BF16)

        def owner(rel, put):
            if c == 0:
                for g in range(groups):
                    wo_copy(device(rel) * groups + g).wait()
            for g in range(groups):
                at = wo_at + (device(rel) * groups + g) * qw
                put(g, product(lambda k, m: seen[r0:r0 + r, k:k + m], lambda k, m: arena[rows(at + k, m), :], qw, qw))

        def put_far(g, t):
            for way in range(2):
                far_terms[way, g, r0:r0 + r, :] = t[:, half_lanes[way]].astype(BF16)

        def put_own(g, t):
            own[g, r0:r0 + r, :] = t

        owner(FAR, put_far)
        for way in range(2):
            chunk_link(0, c, way).start()
        for way in range(2):
            def put_side(g, t):
                side[way, g, r0:r0 + r, :] = t
            owner(to[way], put_side)
        owner(0, put_own)

    def relay(c):
        r0, r = chunks[c]
        for way in range(2):
            chunk_link(0, c, way).wait_recv()

            def block(g, _):
                for lanes in range(2):
                    t = side[way, g, r0:r0 + r, half_lanes[lanes]]
                    if lanes == way:
                        t = t + far_got[way, g, r0:r0 + r, :].astype(F32)
                    terms[way, g, r0:r0 + r, half_lanes[lanes]] = t.astype(BF16)
                return 0
            lax.fori_loop(0, groups, block, 0)
            chunk_link(1, c, way).start()

    def reduce(c):
        r0, r = chunks[c]
        for way in range(2):
            chunk_link(1, c, way).wait_recv()

        def block(g, _):
            s = own[g, r0:r0 + r, :]
            for way in range(2):
                s += got[way, g, r0:r0 + r, :].astype(F32)
            hb[me, g, r0:r0 + r, :] = (x_ref[r0:r0 + r, rows(me * own_cols + g * BN, BN, BN)].astype(F32) + s).astype(BF16)
            return 0
        lax.fori_loop(0, groups, block, 0)
        for way in range(2):
            chunk_link(2, c, way).start()
        if c == len(chunks) - 1:
            chunk_link(3, c, 0).start()

    def forward(c):
        for way in range(2):
            source = device(to[1 - way])
            chunk_link(2, c, way, source).wait_recv()
            chunk_link(3, c, way, source).start()

    wait_keys(0)
    score(0, sc_a)
    last = len(chunks) - 1
    for c, (r0, r) in enumerate(chunks):
        if c:
            attend(r0, r0 + cfg["relay_after"])
            relay(c - 1)
            attend(r0 + cfg["relay_after"], r0 + cfg["reduce_after"])
            reduce(c - 1)
            attend(r0 + cfg["reduce_after"], r0 + r)
        else:
            attend(r0, r0 + r)
            pl.semaphore_wait(barrier, n - 1)
        project(c)
    for t in range(half, 2 * half):
        up_copy(t // 2, t % 2).start()
    def norm_chunk(c):
        r0, r = chunks[c]
        norm_into(lambda o, g: hb[o, g, r0:r0 + r, :], gm_ref, r0, r)

    for c in range(last):
        forward(c)
    relay(last)
    for c in range(last):
        for way in range(2):
            chunk_link(3, c, way).wait_recv()
        norm_chunk(c)
    reduce(last)
    for way in range(2):
        chunk_link(2, last, way).wait_recv()
    chunk_link(3, last, 0).wait_recv()
    norm_chunk(last)
    for c in range(len(chunks)):
        for way in range(2):
            for kind in range(3):
                chunk_link(kind, c, way).wait_send()
        for way in range(2 if c < last else 1):
            chunk_link(3, c, way).wait_send()

    def up(j, _):
        for which in range(2):
            up_copy(j, which).wait()
        gate, value = products(
            lambda k, m: norm[:, k:k + m], [lambda k, m, at=region(2 * j + which): arena[rows(at + k, m), :] for which in range(2)], d, BN)
        hid[:, columns(j)] = (jax.nn.silu(gate) * value).astype(BF16)

        @pl.when(j + half < n_up)
        def _():
            up_copy(j + half, 0).start()
            up_copy(j + half, 1).start()

        for e in range(half):
            @pl.when(j == n_up - half + e)
            def _():
                for v in (2 * e, 2 * e + 1):
                    down_copy(v).start()
        return 0
    lax.fori_loop(0, n_up, up, 0)

    def down(p):
        two = (2 * p, 2 * p + 1)
        for v in two:
            down_copy(v).wait()
        found = products(
            lambda k, m: hid[:, k:k + m], [lambda k, m, at=region(2 * n_up + v): arena[rows(at + k, m), :] for v in two], ff, BN)
        for v in two:
            if v + 2 * half < len(blocks):
                down_copy(v + 2 * half).start()
        return found

    def group_link(kind, g, way, owner=None):
        straight = kind == 3 and g >= groups - 2
        lanes = half_lanes[way] if kind == 3 and not straight else slice(0, BN)
        owner = me if owner is None else owner
        if kind < 2:
            src, dst = ((far_terms, far_got), (terms, got))[kind]
            return link(4 + kind, g, way, src.at[way, g], dst.at[way, g])
        states = yb.at[owner, g, :, lanes]
        return link(4 + kind, g, way, states, states, FAR if straight else None)

    def send_far(t, group):
        for way in range(2):
            far_terms[way, group] = t[:, half_lanes[way]].astype(BF16)
        for way in range(2):
            group_link(0, group, way).start()

    def send_side(t, g, way):
        group_link(0, g, way).wait_recv()
        for lanes in range(2):
            u = t[:, half_lanes[lanes]]
            if lanes == way:
                u = u + far_got[way, g].astype(F32)
            terms[way, g, :, half_lanes[lanes]] = u.astype(BF16)
        group_link(1, g, way).start()

    def finish(g):
        for way in range(2):
            group_link(1, g, way).wait_recv()
        s = own[g]
        for way in range(2):
            s += got[way, g].astype(F32)
        yb[me, g] = (hb[me, g].astype(F32) + s).astype(BF16)
        for way in range(2):
            group_link(2, g, way).start()
        if g >= groups - 2:
            group_link(3, g, 0).start()

    def pass_on(g):
        for way in range(2):
            source = device(to[1 - way])
            group_link(2, g, way, source).wait_recv()
            group_link(3, g, way, source).start()

    sent, done = {}, {}
    for p, two in enumerate(order):
        for (rel, g), t in zip(two, down(p)):
            if rel == FAR:
                send_far(t, g)
            elif rel == OWN:
                own[g] = t
            else:
                send_side(t, g, to.index(rel))
                sent[g] = p
        mine = {g for two_ in order[:p + 1] for rel, g in two_ if rel == OWN}
        for g in range(groups):
            if g in done and done[g] is not None and g < groups - 2 and p >= done[g] + 2:
                pass_on(g)
                done[g] = None
        for g in range(groups):
            if g not in done and g in mine and g in sent and p >= sent[g] + 2:
                finish(g)
                done[g] = p
    for g in range(groups):
        if g not in done:
            finish(g)
            done[g] = len(order)
    for g in range(groups - 2):
        if done[g] is not None:
            pass_on(g)

    for g in range(groups):
        straight = g >= groups - 2
        for way in range(2):
            for kind in range(3):
                group_link(kind, g, way).wait_send()
            if straight:
                group_link(2, g, way).wait_recv()
        for way in range(1 if straight else 2):
            group_link(3, g, way).wait_send()
            group_link(3, g, way).wait_recv()
        for o in range(n):
            y_ref[:, rows(o * own_cols + g * BN, BN, BN)] = yb[o, g]


def solution(mesh):
    n = mesh.shape["tp"]

    def step(x, k_cache, v_cache, gain_a, wq, wo, gain_m, w_gate, w_up, w_down):
        batch, d = x.shape
        cache, kv_heads = k_cache.shape[1:3]
        keys = cache * kv_heads
        heads = wq.shape[1] // HEAD
        ff = w_gate.shape[1]
        half, groups = 7, d // n // BN
        kv_slots = half * d // (2 * keys)
        pairs = batch // 2
        after = []
        for t in range(half):
            r = (t + 3) % half
            need = [s for s in range(kv_slots) if s * 2 * keys < (r + 1) * d and (s + 1) * 2 * keys > r * d]
            after.append(max(p for p in range(pairs - kv_slots, pairs) if p % kv_slots in need))
        chunks = ((0, batch * 3 // 4), (batch * 3 // 4, batch // 4))
        cfg = dict(n=n, batch=batch, d=d, keys=keys, heads=heads, ff=ff, chunks=chunks, relay_after=batch // 16, reduce_after=batch * 3 // 16, after=after)

        i = np.arange(HEAD // 2)
        angle = (cache - 1) * THETA ** (-i / (HEAD // 2))
        cos, sin = np.cos(angle), np.sin(angle)
        turn = jnp.asarray(np.stack([np.concatenate([cos, cos]), np.concatenate([-sin, sin])]), F32)

        any_, vmem = pl.BlockSpec(memory_space=pl.ANY), pl.BlockSpec(memory_space=pltpu.VMEM)
        dma = pltpu.SemaphoreType.DMA
        nc = len(chunks)
        return pl.pallas_call(
            functools.partial(kernel, cfg),
            out_shape=jax.ShapeDtypeStruct(x.shape, x.dtype),
            in_specs=[any_, any_, any_, vmem, any_, any_, vmem, any_, any_, any_, vmem],
            out_specs=vmem,
            scratch_shapes=[
                pltpu.VMEM((2 * half * d, BN), BF16),
                pltpu.VMEM((batch, d), BF16),
                pltpu.VMEM((batch, d), BF16),
                pltpu.VMEM((heads, batch, HEAD), F32),
                pltpu.VMEM((batch * PAD, HEAD), F32),
                pltpu.VMEM((batch * PAD, HEAD), F32),
                pltpu.VMEM((batch, heads * HEAD), BF16),
                pltpu.VMEM((2, groups, batch, BN // 2), BF16),
                pltpu.VMEM((2, groups, batch, BN // 2), BF16),
                pltpu.VMEM((2, groups, batch, BN), F32),
                pltpu.VMEM((2, groups, batch, BN), BF16),
                pltpu.VMEM((2, groups, batch, BN), BF16),
                pltpu.VMEM((groups, batch, BN), F32),
                pltpu.VMEM((n, groups, batch, BN), BF16),
                pltpu.VMEM((batch, ff), BF16),
                pltpu.VMEM((n, groups, batch, BN), BF16),
                pltpu.VMEM((2 * PAD, keys), F32),
                pltpu.VMEM((2 * PAD, keys), F32),
                dma((half + d // BN,)), dma((kv_slots, 4)), dma((1,)),
                *[dma((2, nc))] * 8, *[dma((2, groups))] * 8,
            ],
            compiler_params=pltpu.CompilerParams(collective_id=0, has_side_effects=True, vmem_limit_bytes=67043328),
        )(x, k_cache.reshape(batch, keys, HEAD), v_cache.reshape(batch, keys, HEAD), gain_a.reshape(1, d), wq, wo,
          gain_m.reshape(1, d), w_gate, w_up, w_down, turn)

    states, cache, columns_, rows_of = P("dp", None), P("dp", None, "tp", None), P(None, "tp"), P("tp", None)
    return jax.shard_map(
        step,
        mesh=mesh,
        in_specs=(states, cache, cache, P(None), columns_, rows_of, P(None), columns_, columns_, rows_of),
        out_specs=states,
        check_vma=False,
    )
```

```python
import functools

import jax
import jax.numpy as jnp
import numpy as np
from jax import lax
from jax.experimental import pallas as pl
from jax.experimental.pallas import tpu as pltpu
from jax.sharding import PartitionSpec as P

HEAD = 128
THETA = 10000
MESH = pl.DeviceIdType.MESH
BN = 256
PAD = 16
F32, BF16 = jnp.float32, jnp.bfloat16


def rows(at, size, step=16):
    return pl.ds(pl.multiple_of(at, step), size)


def product(a, w, depth, piece):
    total = None
    for k in range(0, depth, piece):
        term = jnp.dot(a(k, piece), w(k, piece), preferred_element_type=F32)
        total = term if total is None else total + term
    return total


def products(a, ws, depth, piece):
    totals = [None] * len(ws)
    for k in range(0, depth, piece):
        for i, w in enumerate(ws):
            term = jnp.dot(a(k, piece), w(k, piece), preferred_element_type=F32)
            totals[i] = term if totals[i] is None else totals[i] + term
    return totals


def kernel(cfg, x_hbm, k_hbm, v_hbm, ga_ref, wq_hbm, wo_hbm, gm_ref, wg_hbm, wu_hbm, wd_hbm, turn_ref, y_ref,
           arena, x_ref, norm, gain_a, gain_m, qt, qs, os_, seen, far_terms, far_got, side, terms, got, own, hb, hid, yb, sc_a, sc_b,
           blk_sem, kv_sem, x_sem, *link_sems):
    n, batch, d, keys, heads, ff, chunks = cfg["n"], cfg["batch"], cfg["d"], cfg["keys"], cfg["heads"], cfg["ff"], cfg["chunks"]
    qw = heads * HEAD
    own_cols = d // n
    groups = own_cols // BN
    half = 7
    wo_at = half * d
    kv_slots = (half * d) // (2 * keys)
    pairs = batch // 2
    n_up = ff // BN
    me = lax.axis_index("tp")
    scale = HEAD ** -0.5

    FAR, RIGHT, LEFT = 2, 1, n - 1
    to = (RIGHT, LEFT)

    def device(rel):
        return lax.rem(me + rel, n)

    barrier = pltpu.get_barrier_semaphore()
    for rel in range(1, n):
        pl.semaphore_signal(barrier, inc=1, device_id={"tp": device(rel)}, device_id_type=MESH)

    def link(kind, index, way, src, dst, rel=None):
        send, recv = link_sems[2 * kind], link_sems[2 * kind + 1]
        return pltpu.make_async_remote_copy(
            src_ref=src, dst_ref=dst, send_sem=send.at[way, index], recv_sem=recv.at[way, index],
            device_id={"tp": device(to[way] if rel is None else rel)}, device_id_type=MESH)

    def wq_copy(i):
        return pltpu.make_async_copy(wq_hbm.at[:, rows(i * BN, BN, BN)], arena.at[rows(i * d, d), :], blk_sem.at[i])

    def wo_copy(i):
        return pltpu.make_async_copy(wo_hbm.at[:, rows(i * BN, BN, BN)], arena.at[rows(wo_at + i * qw, qw), :], blk_sem.at[half + i])

    def kv_copies(p, kinds=(0, 1)):
        slot = lax.rem(p, kv_slots)
        base = slot * (2 * keys)
        return [
            pltpu.make_async_copy(src.at[2 * p + s], arena.at[rows(base + j * keys, keys), s * HEAD:(s + 1) * HEAD], kv_sem.at[slot, 2 * j + s])
            for j, src in enumerate((k_hbm, v_hbm)) if j in kinds for s in range(2)
        ]

    def region(t):
        r = lax.rem(t, 2 * half)
        return (lax.rem(r + 3, half) + half * (r // half)) * d

    def up_copy(j, which):
        src = (wg_hbm, wu_hbm)[which]
        t = 2 * j + which
        return pltpu.make_async_copy(src.at[:, rows(j * BN, BN, BN)], arena.at[rows(region(t), d), :], blk_sem.at[lax.rem(t, 2 * half)])

    OWN = 0
    half_terms = [(FAR, g) for g in range(groups)] + [(OWN, 0)]
    order = [half_terms[i:i + 2] for i in range(0, groups + 1, 2)]
    for g in range(groups):
        order.append([(RIGHT, g), (LEFT, g)])
        if g % 3 == 1:
            at = g // 3 * 2 + 1
            order.append([(OWN, at), (OWN, at + 1)])
    order.append([(OWN, groups - 2), (OWN, groups - 1)])
    blocks = [b for two in order for b in two]

    def down_copy(v):
        rel, group = blocks[v]
        t = 2 * n_up + v
        src = wd_hbm.at[:, rows((device(rel) * groups + group) * BN, BN, BN)]
        return pltpu.make_async_copy(src, arena.at[rows(region(t), ff), :], blk_sem.at[t % (2 * half)])

    n_wq, n_wo = qw // BN, d // BN
    for i in range(n_wq):
        wq_copy(i).start()
    x_copy = pltpu.make_async_copy(x_hbm, x_ref, x_sem.at[0])
    x_copy.start()

    def columns(c):
        return rows(c * BN, BN, BN)

    def norm_into(read, gain_ref, r0, r):
        def add(o, total):
            for g in range(groups):
                wide = read(o, g).astype(F32)
                sq = wide * wide
                total = total + (sq[:, :128] + sq[:, 128:])
            return total
        total = lax.fori_loop(0, n, add, jnp.zeros((r, 128), F32))
        s = lax.rsqrt(jnp.sum(total, -1, keepdims=True) / d + 1e-6)

        def put(o, _):
            for g in range(groups):
                at = columns(o * groups + g)
                row = (o * groups + g) * (BN // HEAD)
                gain = jnp.concatenate([gain_ref[pl.ds(row + k, 1), :] for k in range(BN // HEAD)], 1)
                norm[r0:r0 + r, at] = (read(o, g).astype(F32) * s * gain).astype(BF16)
            return 0
        lax.fori_loop(0, n, put, 0)

    gain_a[...] = ga_ref[...].astype(F32)
    gain_m[...] = gm_ref[...].astype(F32)
    x_copy.wait()
    norm_into(lambda o, g: x_ref[:, columns(o * groups + g)], gain_a, 0, batch)
    qs[...] = jnp.zeros_like(qs)

    def with_norm(at):
        return product(lambda k, m: norm[:, k:k + m], lambda k, m: arena[rows(at + k, m), :], d, d // 4)

    def query(i, _):
        wq_copy(i).wait()
        q = with_norm(i * d).astype(BF16).astype(F32)
        for s in range(BN // HEAD):
            t = q[:, s * HEAD:(s + 1) * HEAD]
            t = t * turn_ref[0:1, :] + pltpu.roll(t, HEAD // 2, 1) * turn_ref[1:2, :]
            qt[i * (BN // HEAD) + s] = t.astype(BF16).astype(F32)

        @pl.when(i >= 1)
        def _():
            for c in kv_copies(i - 1):
                c.start()

        def more(w, _):
            wo_copy(w).start()
            return 0
        lax.fori_loop(i * (n_wo // n_wq), (i + 1) * (n_wo // n_wq), more, 0)
        return 0

    lax.fori_loop(0, n_wq, query, 0)
    for h in range(heads):
        qs[pl.ds(h, batch, stride=PAD), :] = qt[h]

    row = lax.broadcasted_iota(jnp.int32, (2 * PAD, 512), 0)
    lane = lax.broadcasted_iota(jnp.int32, (2 * PAD, 512), 1)
    in_second = (lax.rem(row, PAD) >= heads // 2).astype(jnp.int32)
    bias = jnp.where(lax.rem(lane, 2) == in_second, 0.0, -jnp.inf).astype(F32)
    first = lax.broadcasted_iota(jnp.int32, (2 * PAD, HEAD), 0) < PAD
    width = 512

    def kv_base(p):
        return lax.rem(p, kv_slots) * (2 * keys)

    def wait_keys(p):
        for c in kv_copies(p, (0,)):
            c.wait()

    def wait_values(p):
        for c in kv_copies(p, (1,)):
            c.wait()

    def score(p, sc):
        q = qs[rows(p * (2 * PAD), 2 * PAD), :]
        q = jnp.concatenate([jnp.where(first, q, 0.0), jnp.where(first, 0.0, q)], 1).astype(BF16)
        for c in range(0, keys, width):
            s = lax.dot_general(q, arena[rows(kv_base(p) + c, width), :], (((1,), (1,)), ((), ())), preferred_element_type=F32)
            sc[:, c:c + width] = s * scale + bias

    def see(p, sc):
        top = None
        for c in range(0, keys, width):
            s = sc[:, c:c + width]
            top = s if top is None else jnp.maximum(top, s)
        top = jnp.max(top, -1, keepdims=True)
        total = None
        for c in range(0, keys, width):
            e = jnp.exp(sc[:, c:c + width] - top)
            sc[:, c:c + width] = e
            total = e if total is None else total + e
        inv = 1.0 / jnp.sum(total, -1, keepdims=True)
        o = None
        for c in range(0, keys, BN):
            w = (sc[:, c:c + BN] * inv).astype(BF16)
            t = jnp.dot(w, arena[rows(kv_base(p) + keys + c, BN), :], preferred_element_type=F32)
            o = t if o is None else o + t
        os_[rows(p * (2 * PAD), 2 * PAD), :] = jnp.concatenate([o[:PAD, :HEAD], o[PAD:, HEAD:]], 0)

    def two_pairs(i, end):
        p = 2 * i
        wait_keys(p + 1)
        wait_values(p)
        wait_values(p + 1)
        if not end:
            wait_keys(p + 2)
        score(p + 1, sc_b)
        see(p, sc_a)
        if not end:
            score(p + 2, sc_a)
        see(p + 1, sc_b)

        if not end:
            @pl.when(p + 1 + kv_slots < pairs)
            def _():
                for c in kv_copies(p + kv_slots) + kv_copies(p + 1 + kv_slots):
                    c.start()

        for t, after in enumerate(cfg["after"]):
            if end:
                if after // 2 == i:
                    up_copy(t // 2, t % 2).start()
            elif after // 2 < pairs // 2 - 1:
                @pl.when(i == after // 2)
                def _():
                    up_copy(t // 2, t % 2).start()

    def attend(first_row, last_row):
        def step(i, _):
            two_pairs(i, False)
            return 0
        lo, hi = first_row // 4, last_row // 4
        lax.fori_loop(lo, min(hi, pairs // 2 - 1), step, 0)
        if hi == pairs // 2:
            two_pairs(hi - 1, True)

    half_lanes = (slice(0, BN // 2), slice(BN // 2, BN))

    def chunk_link(kind, c, way, owner=None):
        r0, r = chunks[c]
        straight = kind == 3 and c == len(chunks) - 1
        lanes = half_lanes[way] if kind == 3 and not straight else slice(0, BN)
        owner = me if owner is None else owner

        def at(ref, first=way):
            return ref.at[first, :, r0:r0 + r]
        if kind < 2:
            src, dst = ((far_terms, far_got), (terms, got))[kind]
            return link(kind, c, way, at(src), at(dst))
        states = hb.at[owner, :, r0:r0 + r, lanes]
        return link(kind, c, way, states, states, FAR if straight else None)

    def project(c):
        r0, r = chunks[c]
        for h in range(heads):
            seen[r0:r0 + r, h * HEAD:(h + 1) * HEAD] = os_[pl.ds(r0 * PAD + h, r, stride=PAD), :].astype(BF16)

        def owner(rel, put):
            if c == 0:
                for g in range(groups):
                    wo_copy(device(rel) * groups + g).wait()
            for g in range(groups):
                at = wo_at + (device(rel) * groups + g) * qw
                put(g, product(lambda k, m: seen[r0:r0 + r, k:k + m], lambda k, m: arena[rows(at + k, m), :], qw, qw))

        def put_far(g, t):
            for way in range(2):
                far_terms[way, g, r0:r0 + r, :] = t[:, half_lanes[way]].astype(BF16)

        def put_own(g, t):
            own[g, r0:r0 + r, :] = t

        owner(FAR, put_far)
        for way in range(2):
            chunk_link(0, c, way).start()
        for way in range(2):
            def put_side(g, t):
                side[way, g, r0:r0 + r, :] = t
            owner(to[way], put_side)
        owner(0, put_own)

    def relay(c):
        r0, r = chunks[c]
        for way in range(2):
            chunk_link(0, c, way).wait_recv()

            def block(g, _):
                for lanes in range(2):
                    t = side[way, g, r0:r0 + r, half_lanes[lanes]]
                    if lanes == way:
                        t = t + far_got[way, g, r0:r0 + r, :].astype(F32)
                    terms[way, g, r0:r0 + r, half_lanes[lanes]] = t.astype(BF16)
                return 0
            lax.fori_loop(0, groups, block, 0)
            chunk_link(1, c, way).start()

    def reduce(c):
        r0, r = chunks[c]
        for way in range(2):
            chunk_link(1, c, way).wait_recv()

        def block(g, _):
            s = own[g, r0:r0 + r, :]
            for way in range(2):
                s += got[way, g, r0:r0 + r, :].astype(F32)
            hb[me, g, r0:r0 + r, :] = (x_ref[r0:r0 + r, rows(me * own_cols + g * BN, BN, BN)].astype(F32) + s).astype(BF16)
            return 0
        lax.fori_loop(0, groups, block, 0)
        for way in range(2):
            chunk_link(2, c, way).start()
        if c == len(chunks) - 1:
            chunk_link(3, c, 0).start()

    def forward(c):
        for way in range(2):
            source = device(to[1 - way])
            chunk_link(2, c, way, source).wait_recv()
            chunk_link(3, c, way, source).start()

    wait_keys(0)
    score(0, sc_a)
    last = len(chunks) - 1
    for c, (r0, r) in enumerate(chunks):
        if c:
            attend(r0, r0 + cfg["relay_after"])
            relay(c - 1)
            attend(r0 + cfg["relay_after"], r0 + cfg["reduce_after"])
            reduce(c - 1)
            attend(r0 + cfg["reduce_after"], r0 + r)
        else:
            attend(r0, r0 + r)
            pl.semaphore_wait(barrier, n - 1)
        project(c)
    for t in range(half, 2 * half):
        up_copy(t // 2, t % 2).start()
    def norm_chunk(c):
        r0, r = chunks[c]
        norm_into(lambda o, g: hb[o, g, r0:r0 + r, :], gain_m, r0, r)

    for c in range(last):
        forward(c)
    relay(last)
    for c in range(last):
        for way in range(2):
            chunk_link(3, c, way).wait_recv()
        norm_chunk(c)
    reduce(last)
    for way in range(2):
        chunk_link(2, last, way).wait_recv()
    chunk_link(3, last, 0).wait_recv()
    norm_chunk(last)
    for c in range(len(chunks)):
        for way in range(2):
            for kind in range(3):
                chunk_link(kind, c, way).wait_send()
        for way in range(2 if c < last else 1):
            chunk_link(3, c, way).wait_send()

    def up(j, _):
        for which in range(2):
            up_copy(j, which).wait()
        gate, value = products(
            lambda k, m: norm[:, k:k + m], [lambda k, m, at=region(2 * j + which): arena[rows(at + k, m), :] for which in range(2)], d, BN)
        hid[:, columns(j)] = (jax.nn.silu(gate) * value).astype(BF16)

        @pl.when(j + half < n_up)
        def _():
            up_copy(j + half, 0).start()
            up_copy(j + half, 1).start()

        for e in range(half):
            @pl.when(j == n_up - half + e)
            def _():
                for v in (2 * e, 2 * e + 1):
                    down_copy(v).start()
        return 0
    lax.fori_loop(0, n_up, up, 0)

    def down(p):
        two = (2 * p, 2 * p + 1)
        for v in two:
            down_copy(v).wait()
        found = products(
            lambda k, m: hid[:, k:k + m], [lambda k, m, at=region(2 * n_up + v): arena[rows(at + k, m), :] for v in two], ff, BN)
        for v in two:
            if v + 2 * half < len(blocks):
                down_copy(v + 2 * half).start()
        return found

    def group_link(kind, g, way, owner=None):
        straight = kind == 3 and g >= groups - 2
        lanes = half_lanes[way] if kind == 3 and not straight else slice(0, BN)
        owner = me if owner is None else owner
        if kind < 2:
            src, dst = ((far_terms, far_got), (terms, got))[kind]
            return link(4 + kind, g, way, src.at[way, g], dst.at[way, g])
        states = yb.at[owner, g, :, lanes]
        return link(4 + kind, g, way, states, states, FAR if straight else None)

    def send_far(t, group):
        for way in range(2):
            far_terms[way, group] = t[:, half_lanes[way]].astype(BF16)
        for way in range(2):
            group_link(0, group, way).start()

    def send_side(t, g, way):
        group_link(0, g, way).wait_recv()
        for lanes in range(2):
            u = t[:, half_lanes[lanes]]
            if lanes == way:
                u = u + far_got[way, g].astype(F32)
            terms[way, g, :, half_lanes[lanes]] = u.astype(BF16)
        group_link(1, g, way).start()

    def finish(g):
        for way in range(2):
            group_link(1, g, way).wait_recv()
        s = own[g]
        for way in range(2):
            s += got[way, g].astype(F32)
        yb[me, g] = (hb[me, g].astype(F32) + s).astype(BF16)
        for way in range(2):
            group_link(2, g, way).start()
        if g >= groups - 2:
            group_link(3, g, 0).start()

    def pass_on(g):
        for way in range(2):
            source = device(to[1 - way])
            group_link(2, g, way, source).wait_recv()
            group_link(3, g, way, source).start()

    sent, done = {}, {}
    for p, two in enumerate(order):
        for (rel, g), t in zip(two, down(p)):
            if rel == FAR:
                send_far(t, g)
            elif rel == OWN:
                own[g] = t
            else:
                send_side(t, g, to.index(rel))
                sent[g] = p
        mine = {g for two_ in order[:p + 1] for rel, g in two_ if rel == OWN}
        for g in range(groups):
            if g in done and done[g] is not None and g < groups - 2 and p >= done[g] + 2:
                pass_on(g)
                done[g] = None
        for g in range(groups):
            if g not in done and g in mine and g in sent and p >= sent[g] + 2:
                finish(g)
                done[g] = p
    for g in range(groups):
        if g not in done:
            finish(g)
            done[g] = len(order)
    for g in range(groups - 2):
        if done[g] is not None:
            pass_on(g)

    for g in range(groups):
        straight = g >= groups - 2
        for way in range(2):
            for kind in range(3):
                group_link(kind, g, way).wait_send()
            if straight:
                group_link(2, g, way).wait_recv()
        for way in range(1 if straight else 2):
            group_link(3, g, way).wait_send()
            group_link(3, g, way).wait_recv()
        for o in range(n):
            y_ref[:, rows(o * own_cols + g * BN, BN, BN)] = yb[o, g]


def solution(mesh):
    n = mesh.shape["tp"]

    def step(x, k_cache, v_cache, gain_a, wq, wo, gain_m, w_gate, w_up, w_down):
        batch, d = x.shape
        cache, kv_heads = k_cache.shape[1:3]
        keys = cache * kv_heads
        heads = wq.shape[1] // HEAD
        ff = w_gate.shape[1]
        half, groups = 7, d // n // BN
        kv_slots = half * d // (2 * keys)
        pairs = batch // 2
        after = []
        for t in range(half):
            r = (t + 3) % half
            need = [s for s in range(kv_slots) if s * 2 * keys < (r + 1) * d and (s + 1) * 2 * keys > r * d]
            after.append(max(p for p in range(pairs - kv_slots, pairs) if p % kv_slots in need))
        chunks = ((0, batch * 3 // 4), (batch * 3 // 4, batch // 4))
        cfg = dict(n=n, batch=batch, d=d, keys=keys, heads=heads, ff=ff, chunks=chunks, relay_after=batch // 16, reduce_after=batch * 3 // 16, after=after)

        i = np.arange(HEAD // 2)
        angle = (cache - 1) * THETA ** (-i / (HEAD // 2))
        cos, sin = np.cos(angle), np.sin(angle)
        turn = jnp.asarray(np.stack([np.concatenate([cos, cos]), np.concatenate([-sin, sin])]), F32)

        any_, vmem = pl.BlockSpec(memory_space=pl.ANY), pl.BlockSpec(memory_space=pltpu.VMEM)
        dma = pltpu.SemaphoreType.DMA
        nc = len(chunks)
        return pl.pallas_call(
            functools.partial(kernel, cfg),
            out_shape=jax.ShapeDtypeStruct(x.shape, x.dtype),
            in_specs=[any_, any_, any_, vmem, any_, any_, vmem, any_, any_, any_, vmem],
            out_specs=vmem,
            scratch_shapes=[
                pltpu.VMEM((2 * half * d, BN), BF16),
                pltpu.VMEM((batch, d), BF16),
                pltpu.VMEM((batch, d), BF16),
                pltpu.VMEM((d // HEAD, HEAD), F32),
                pltpu.VMEM((d // HEAD, HEAD), F32),
                pltpu.VMEM((heads, batch, HEAD), F32),
                pltpu.VMEM((batch * PAD, HEAD), F32),
                pltpu.VMEM((batch * PAD, HEAD), F32),
                pltpu.VMEM((batch, heads * HEAD), BF16),
                pltpu.VMEM((2, groups, batch, BN // 2), BF16),
                pltpu.VMEM((2, groups, batch, BN // 2), BF16),
                pltpu.VMEM((2, groups, batch, BN), F32),
                pltpu.VMEM((2, groups, batch, BN), BF16),
                pltpu.VMEM((2, groups, batch, BN), BF16),
                pltpu.VMEM((groups, batch, BN), F32),
                pltpu.VMEM((n, groups, batch, BN), BF16),
                pltpu.VMEM((batch, ff), BF16),
                pltpu.VMEM((n, groups, batch, BN), BF16),
                pltpu.VMEM((2 * PAD, keys), F32),
                pltpu.VMEM((2 * PAD, keys), F32),
                dma((half + d // BN,)), dma((kv_slots, 4)), dma((1,)),
                *[dma((2, nc))] * 8, *[dma((2, groups))] * 8,
            ],
            compiler_params=pltpu.CompilerParams(collective_id=0, has_side_effects=True, vmem_limit_bytes=67043328),
        )(x, k_cache.reshape(batch, keys, HEAD), v_cache.reshape(batch, keys, HEAD), gain_a.reshape(d // HEAD, HEAD), wq, wo,
          gain_m.reshape(d // HEAD, HEAD), w_gate, w_up, w_down, turn)

    states, cache, columns_, rows_of = P("dp", None), P("dp", None, "tp", None), P(None, "tp"), P("tp", None)
    return jax.shard_map(
        step,
        mesh=mesh,
        in_specs=(states, cache, cache, P(None), columns_, rows_of, P(None), columns_, columns_, rows_of),
        out_specs=states,
        check_vma=False,
    )
```
